32 devices in a mesh: pb: 4 (over y, core), pa: 8 (over z, x).
Axes of the slice: x: 2, y: 2, z: 4, core: 2. Of those that a mesh axis runs over, the one named last changes fastest.
Arguments:
- query_hidden: bfloat16 [32, 32, 2048], P('pb', 'pa'), may hold values from -32 to 32
- page_hidden: bfloat16 [8, 1024, 2048], P('pa', 'pb'), may hold values from -4.2 to 4.2
- projection: bfloat16 [2048, 128], replicated, may hold values from -0.125 to 0.125
- clicks: int32 [32, 8, 2], P('pb'), may hold values from 0 to 7, as said below
- bins: int32 [32, 8], P('pb'), may hold values from 0 to 7
Outputs:
- query_grad: bfloat16 [32, 32, 2048], P('pb', 'pa')
- page_grad: bfloat16 [8, 1024, 2048], P('pa', 'pb')
- weight_grad: float32 [2048, 128], P(('pb', 'pa'))
The draws below stay inside these ranges and needn't reach their ends.
Inputs may be any that keep to these rules, and one draw needn't show every extreme that they name: `clicks`: the two pages of a pair always differ.
All inputs are finite; a program needn't handle non-finite values.
Results may differ from the reference program's by a relative error of at most 0.019.
Values may be sent and summed in bfloat16 or wider, within the bound.
A program may use at most 64 MiB of HBM per device.

```python
import jax
import jax.numpy as jnp
from jax import lax

D = 2048
E = 128
NPATCH = 1024
LQ = 32
PAIRS = 8
BINS = 8
NQ = 32
NP = 8


def query_base(key):
    return jax.random.truncated_normal(jax.random.fold_in(key, 1), -4.0, 4.0, (NQ, LQ, D), jnp.float32)


def draw_query_hidden(key, part):
    values = query_base(key)
    return values.astype(jnp.bfloat16)


def draw_page_hidden(key, part):
    values = jax.random.truncated_normal(jax.random.fold_in(key, 2), -4.0, 4.0, (NP, NPATCH, D), jnp.float32)
    return values.astype(jnp.bfloat16)


def draw_clicks(key, part):
    positive = jax.random.randint(jax.random.fold_in(key, 3), (NQ, PAIRS), 0, NP)
    offset = jax.random.randint(jax.random.fold_in(key, 4), (NQ, PAIRS), 1, NP)
    negative = (positive + offset) % NP
    return jnp.stack([positive, negative], axis=2).astype(jnp.int32)


def place_ends(values, own_key, low, high):
    index_at = [jax.random.randint(jax.random.fold_in(own_key, axis), (), 0, length) for axis, length in enumerate(values.shape)]
    main_axis = values.shape.index(max(values.shape))
    neighbour = index_at[:main_axis] + [(index_at[main_axis] + 1) % values.shape[main_axis]] + index_at[main_axis + 1:]
    return values.at[tuple(index_at)].set(low).at[tuple(neighbour)].set(high)


def noise(rng, extent, spread, reach, kind=jnp.bfloat16):
    drawn = spread * jax.random.normal(rng, extent, jnp.float32)
    return jnp.clip(drawn, min=-reach, max=reach).astype(kind)


def setup_inputs(seed: int = 0) -> dict:
    splits = jax.random.split(jax.random.key(seed), 6)
    return {
        "query_hidden": draw_query_hidden(jax.random.fold_in(splits[5], 71), 0),
        "page_hidden": draw_page_hidden(jax.random.fold_in(splits[5], 71), 0),
        "projection": noise(splits[2], (D, E), D ** -0.5, 0.125),
        "clicks": draw_clicks(jax.random.fold_in(splits[5], 71), 0),
        "bins": place_ends(jax.random.randint(splits[4], (NQ, PAIRS), 0, BINS), jax.random.fold_in(splits[4], 1), 0, BINS - 1).astype(jnp.int32),
    }


sharpness = 0.25

def reference(query_hidden, page_hidden, projection, clicks, bins):
    hidden_width = query_hidden.shape[2]
    query_embed = jnp.dot(query_hidden.reshape(-1, hidden_width), projection, preferred_element_type=jnp.float32).astype(jnp.bfloat16)
    page_embed = jnp.dot(page_hidden.reshape(-1, hidden_width), projection, preferred_element_type=jnp.float32).astype(jnp.bfloat16).reshape(NP, NPATCH, E)

    def page_norm(page_block):
        logit_block = sharpness * jnp.dot(query_embed, page_block.T, preferred_element_type=jnp.float32)
        return jax.nn.logsumexp(logit_block, axis=1)
    log_norm = lax.map(page_norm, page_embed)
    query_score = log_norm.T.reshape(NQ, LQ, NP).sum(axis=1)
    page_ids = jnp.arange(NP, dtype=jnp.int32)
    hit_pos = (clicks[:, :, 0][:, :, None] == page_ids).astype(jnp.float32)
    hit_neg = (clicks[:, :, 1][:, :, None] == page_ids).astype(jnp.float32)
    pair_gap = lax.optimization_barrier(jnp.sum(hit_pos * query_score[:, None, :], axis=2)) - lax.optimization_barrier(jnp.sum(hit_neg * query_score[:, None, :], axis=2))
    pair_weight = jnp.sqrt(bins.astype(jnp.float32) + 1.0)
    pair_coeff = -pair_weight * jax.nn.sigmoid(-pair_gap)
    score_grad = lax.optimization_barrier(jnp.sum(pair_coeff[:, :, None] * (hit_pos - hit_neg), axis=1))
    grad_rows = jnp.repeat(score_grad, LQ, axis=0)

    def page_back(token_acc, inputs):
        page_block, norm_col, grad_col = inputs
        logit_block = sharpness * jnp.dot(query_embed, page_block.T, preferred_element_type=jnp.float32)
        soft_grad = (grad_col[:, None] * jnp.exp(logit_block - norm_col[:, None])).astype(jnp.bfloat16)
        token_acc = token_acc + jnp.dot(soft_grad, page_block, preferred_element_type=jnp.float32)
        patch_part = jnp.dot(soft_grad.T, query_embed, preferred_element_type=jnp.float32)
        return (token_acc, patch_part)
    token_acc, patch_acc = lax.scan(page_back, jnp.zeros((NQ * LQ, E), jnp.float32), (page_embed, log_norm, grad_rows.T))
    token_low = (sharpness * token_acc).astype(jnp.bfloat16)
    patch_low = (sharpness * patch_acc).astype(jnp.bfloat16).reshape(-1, E)
    query_grad = jnp.dot(token_low, projection.T, preferred_element_type=jnp.float32).astype(jnp.bfloat16).reshape(query_hidden.shape)
    page_grad = jnp.dot(patch_low, projection.T, preferred_element_type=jnp.float32).astype(jnp.bfloat16).reshape(page_hidden.shape)
    weight_grad = jnp.dot(query_hidden.reshape(-1, hidden_width).T, token_low, preferred_element_type=jnp.float32)
    weight_grad = weight_grad + jnp.dot(page_hidden.reshape(-1, hidden_width).T, patch_low, preferred_element_type=jnp.float32)
    return (query_grad, page_grad, weight_grad)
```

```python
import functools
import math

import jax
import jax.numpy as jnp
from jax import lax
from jax.experimental import pallas as pl
from jax.experimental.pallas import tpu as pltpu
from jax.sharding import PartitionSpec as P

sharpness = 0.25
MESH = pl.DeviceIdType.MESH
BF = jnp.bfloat16
F32 = jnp.float32
FOLDED = sharpness * math.log2(math.e)
LOADS = 5
KINDS = ("query", "click", "bin", "page", "hidden", "raw", "norm", "token", "patch", "low", "weight")


def dot(x, y, dims):
    return lax.dot_general(x, y, (dims, ((), ())), preferred_element_type=F32)


def kernel(
    PB, PA, qh_hbm, ph_hbm, proj_hbm, clicks_hbm, bins_hbm,
    qg_ref, pg_ref, w_ref,
    clicks_ref, bins_ref, qraw, qh, qb, qx, ph, hx, pht, proj, qe, qt, pe, lbuf, ebuf, norm,
    tsend, trecv, gsend, grecv, low, wq, wsend, wrecv, sems,
):
    b = lax.axis_index("pb")
    a = lax.axis_index("pa")
    queries, token_local, hidden = qh_hbm.shape
    rows = queries * token_local
    patches = ph_hbm.shape[0]
    E = proj.shape[1]
    half = PB // 2
    slots = half * PA
    tokens = slots * rows
    total_queries = half * queries
    parity = lax.rem(b, 2)
    level = b // 2
    me = level * PA + a
    partner = (b + 1 - 2 * parity, a)
    chunk = w_ref.shape[0]
    span = PA * chunk
    width = 2 if PA < 32 else 4
    deep = PA // width
    z = a // width
    x = lax.rem(a, width)
    upper = z >= deep // 2

    def sem(kind, receive):
        return sems.at[LOADS + 2 * KINDS.index(kind) + receive]

    def remote(kind, src, dst, to):
        c = pltpu.make_async_remote_copy(
            src_ref=src, dst_ref=dst, send_sem=sem(kind, 0), recv_sem=sem(kind, 1),
            device_id=to, device_id_type=MESH,
        )
        c.start()

    def drain(kind, ref, receive):
        pltpu.make_async_copy(ref, ref, sem(kind, receive)).wait()

    def others(offsets):
        for i in range(deep):
            far = jnp.where(upper, i, deep - 1 - i)
            for k in offsets:
                to_level = lax.rem(level + k, half)
                for j in list(range(1, width)) + [0]:
                    to_z = far
                    if k == 0 and j == 0:
                        if i == deep - 1:
                            continue
                        up = i + jnp.where(i >= z, 1, 0)
                        down = deep - 1 - i - jnp.where(deep - 1 - i <= z, 1, 0)
                        to_z = jnp.where(upper, up, down)
                    yield to_level, to_z * width + lax.rem(x + j, width)

    every = list(range(1, half)) + [0]

    def device(to_level, to_a):
        return 2 * to_level + parity, to_a

    loads = [
        pltpu.make_async_copy(qh_hbm, qraw, sems.at[0]),
        pltpu.make_async_copy(proj_hbm, proj, sems.at[1]),
        pltpu.make_async_copy(ph_hbm, ph, sems.at[2]),
        pltpu.make_async_copy(clicks_hbm, clicks_ref.at[level], sems.at[3]),
        pltpu.make_async_copy(bins_hbm, bins_ref.at[level], sems.at[4]),
    ]
    for c in loads:
        c.start()
    barrier = pltpu.get_barrier_semaphore()
    for to in others(every):
        pl.semaphore_signal(barrier, inc=1, device_id=device(*to), device_id_type=MESH)
    pl.semaphore_signal(barrier, inc=1, device_id=partner, device_id_type=MESH)

    loads[0].wait()
    for q in range(queries):
        qh[q * token_local:(q + 1) * token_local] = qraw[q].astype(F32)
    qb[...] = qh[...].astype(BF)
    loads[1].wait()
    qe[me] = dot(qb[...], proj[...], ((1,), (0,))).astype(BF)
    pl.semaphore_wait(barrier, slots)
    for to in others(every):
        remote("query", qe.at[me], qe.at[me], device(*to))
    for k in range(1, half):
        to = device(lax.rem(level + k, half), a)
        remote("click", clicks_hbm, clicks_ref.at[level], to)
        remote("bin", bins_hbm, bins_ref.at[level], to)

    loads[2].wait()
    pe[0] = dot(ph[...], proj[...], ((1,), (0,))).astype(BF)
    remote("page", pe.at[0], pe.at[1], partner)

    def columns(l, core):
        return pl.ds(pl.multiple_of((2 * l + core) * span, 128), span)

    for l in range(half):
        remote("hidden", ph.at[:, columns(l, 1 - parity)], hx.at[l], partner)
        remote("raw", qb.at[:, columns(l, 1 - parity)], qx.at[l], partner)

    query_of = lax.broadcasted_iota(jnp.int32, (total_queries, tokens), 0)
    token_of = lax.broadcasted_iota(jnp.int32, (total_queries, tokens), 1)

    def belongs(query_id, token_id):
        own_query = lax.rem(token_id, rows) // token_local + token_id // (PA * rows) * queries
        return jnp.where(query_id == own_query, 1.0, 0.0)

    mask = belongs(query_of, token_of)
    for l in range(half):
        pht[l, 0] = ph[:, columns(l, parity)].T
    drain("hidden", hx, 1)
    for l in range(half):
        pht[l, 1] = hx[l].T

    drain("page", pe.at[0], 1)
    drain("query", qe.at[pl.ds(0, slots - 1)], 1)
    tok = qe[...].reshape(tokens, E)
    top = None
    for k in range(2):
        block = dot(pe[k], tok, ((1,), (1,)))
        lbuf[k] = block
        high = jnp.max(block, axis=0, keepdims=True)
        top = high if top is None else jnp.maximum(top, high)
    total = None
    for k in range(2):
        e = jnp.exp2((lbuf[k] - top) * FOLDED)
        ebuf[k] = e.astype(BF)
        part = jnp.sum(e, axis=0, keepdims=True)
        total = part if total is None else total + part
    top = sharpness * top
    norm[me] = top + jnp.log(total)
    for to in others(every):
        remote("norm", norm.at[me], norm.at[me], device(*to))

    unit = dot(pe[0], ebuf[0], ((0,), (0,))) + dot(pe[1], ebuf[1], ((0,), (0,)))
    unit = (unit / total).T.astype(BF)
    for s in range(slots):
        tsend[s] = unit[s * rows:(s + 1) * rows]
    for to_level, to_a in others(every):
        remote("token", tsend.at[to_level * PA + to_a], trecv.at[me], device(to_level, to_a))
    trecv[me] = tsend[me]
    qt[...] = tok.astype(F32).T

    loads[3].wait()
    loads[4].wait()
    if half > 1:
        drain("click", clicks_ref.at[pl.ds(0, half - 1)], 1)
        drain("bin", bins_ref.at[pl.ds(0, half - 1)], 1)
    pairs = bins_ref.shape[2]
    pos = clicks_ref[:, :, 0, :].reshape(total_queries, pairs)
    neg = clicks_ref[:, :, 1, :].reshape(total_queries, pairs)
    weight = jnp.sqrt(bins_ref[...].reshape(total_queries, pairs).astype(F32) + 1.0)

    def merged(parts):
        high = functools.reduce(jnp.maximum, parts)
        return high + jnp.log(functools.reduce(jnp.add, [jnp.exp(v - high) for v in parts]))

    drain("norm", norm.at[pl.ds(0, slots - 1)], 1)
    at_pos = jnp.zeros(pos.shape, F32)
    at_neg = jnp.zeros(pos.shape, F32)
    for p in range(PA):
        log_norm = merged([norm[l * PA + p] for l in range(half)])
        score = jnp.sum(mask * log_norm, axis=1, keepdims=True)
        at_pos = at_pos + jnp.where(pos == p, score, 0.0)
        at_neg = at_neg + jnp.where(neg == p, score, 0.0)
    coeff = -weight * jax.nn.sigmoid(at_neg - at_pos)

    def score_grad(page):
        hits = (pos == page).astype(F32) - (neg == page).astype(F32)
        return jnp.sum(coeff * hits, axis=1, keepdims=True)

    log_norm = merged([norm[l * PA + a] for l in range(half)])
    factor = jnp.sum(mask * score_grad(a), axis=0, keepdims=True) * jnp.exp(top - log_norm)
    scaled = (qt[...] * factor).astype(BF)
    mine = []
    for k in range(2):
        part = dot(scaled, ebuf[k], ((1,), (1,)))
        gsend[k] = part.astype(BF)
        mine.append(part)
    remote("patch", gsend, grecv, partner)

    lanes = min(128, tokens)
    near = pl.ds(pl.multiple_of(me * rows // lanes * lanes, lanes), lanes)
    first = me * rows // lanes * lanes
    own_mask = belongs(
        lax.broadcasted_iota(jnp.int32, (total_queries, lanes), 0),
        first + lax.broadcasted_iota(jnp.int32, (total_queries, lanes), 1),
    )
    pick = jnp.where(
        lax.broadcasted_iota(jnp.int32, (rows, lanes), 0) + (me * rows - first)
        == lax.broadcasted_iota(jnp.int32, (rows, lanes), 1), 1.0, 0.0,
    )
    drain("token", trecv.at[pl.ds(0, slots - 1)], 1)
    token_own = None
    for p in range(PA):
        parts = [norm[l * PA + p, :, near] for l in range(half)]
        log_norm = merged(parts)
        grad = jnp.sum(own_mask * score_grad(p), axis=0, keepdims=True)
        for l in range(half):
            share = jnp.sum(pick * (grad * jnp.exp(parts[l] - log_norm)), axis=1, keepdims=True)
            part = trecv[l * PA + p].astype(F32) * share
            token_own = part if token_own is None else token_own + part
    token_low = (sharpness * token_own).astype(BF)
    low[0] = token_low
    remote("low", low.at[0], low.at[1], partner)

    drain("raw", qx, 1)
    drain("low", low.at[0], 1)
    for l in range(half):
        wq[l] = dot(qb[:, columns(l, parity)], token_low, ((0,), (0,))) + dot(qx[l], low[1], ((0,), (0,)))

    drain("patch", grecv, 1)
    patch_low = [(sharpness * (mine[k] + grecv[1 - k].astype(F32))).astype(BF) for k in range(2)]

    for k in every:
        to_level = lax.rem(level + k, half)
        block = wq[to_level]
        for i in range(2):
            block = block + dot(pht[to_level, i], patch_low[i], ((1,), (1,)))
        block = block.astype(BF)
        for s in range(PA):
            wsend[to_level * PA + s] = block[s * chunk:(s + 1) * chunk]
        for _, to_a in others([k]):
            remote("weight", wsend.at[to_level * PA + to_a], wrecv.at[me], device(to_level, to_a))
    wrecv[me] = wsend[me]

    qgrad = dot(token_low, proj[...], ((1,), (1,)))
    for q in range(queries):
        qg_ref[q] = qgrad[q * token_local:(q + 1) * token_local].astype(BF)
    pg_ref[...] = dot(patch_low[0].T, proj[...], ((1,), (1,))).astype(BF)

    drain("query", qe.at[pl.ds(0, slots - 1)], 0)
    if half > 1:
        drain("click", clicks_ref.at[pl.ds(0, half - 1)], 0)
        drain("bin", bins_ref.at[pl.ds(0, half - 1)], 0)
    drain("page", pe.at[0], 0)
    drain("hidden", hx, 0)
    drain("raw", qx, 0)
    drain("norm", norm.at[pl.ds(0, slots - 1)], 0)
    drain("token", tsend.at[pl.ds(0, slots - 1)], 0)
    drain("patch", gsend, 0)
    drain("low", low.at[0], 0)
    drain("weight", wsend.at[pl.ds(0, slots - 1)], 0)
    drain("weight", wrecv.at[pl.ds(0, slots - 1)], 1)
    weight_sum = wrecv[0].astype(F32)
    for s in range(1, slots):
        weight_sum = weight_sum + wrecv[s].astype(F32)
    w_ref[...] = weight_sum


def writer(qg, pg, w, qg_out, pg_out, w_out, sems):
    copies = [
        pltpu.make_async_copy(pg, pg_out, sems.at[0]),
        pltpu.make_async_copy(qg, qg_out, sems.at[1]),
        pltpu.make_async_copy(w, w_out, sems.at[2]),
    ]
    for c in copies:
        c.start()
    for c in copies:
        c.wait()


def shards(PB, PA, query_hidden, page_hidden, projection, clicks, bins):
    queries, token_local, hidden = query_hidden.shape
    page_count, patches, _ = page_hidden.shape
    assert page_count == 1 and PB % 2 == 0
    E = projection.shape[1]
    rows = queries * token_local
    half = PB // 2
    slots = half * PA
    tokens = rows * slots
    chunk = hidden // (PB * PA)
    span = PA * chunk
    pairs = clicks.shape[1]
    ph = page_hidden.reshape(patches, hidden)
    vmem = pl.BlockSpec(memory_space=pltpu.VMEM)
    hbm = pl.BlockSpec(memory_space=pltpu.HBM)
    dma = lambda n: pltpu.SemaphoreType.DMA((n,))
    outs = (
        jax.ShapeDtypeStruct(query_hidden.shape, BF),
        jax.ShapeDtypeStruct((patches, hidden), BF),
        jax.ShapeDtypeStruct((chunk, E), F32),
    )
    results = pl.pallas_call(
        functools.partial(kernel, PB, PA),
        out_shape=tuple(pltpu.VMEM(o.shape, o.dtype) for o in outs),
        in_specs=[hbm] * 5,
        out_specs=(vmem,) * 3,
        scratch_shapes=[
            pltpu.VMEM((half, queries, 2, pairs), jnp.int32),
            pltpu.VMEM((half, queries, pairs), jnp.int32),
            pltpu.VMEM(query_hidden.shape, BF),
            pltpu.VMEM((rows, hidden), F32),
            pltpu.VMEM((rows, hidden), BF),
            pltpu.VMEM((half, rows, span), BF),
            pltpu.VMEM((patches, hidden), BF),
            pltpu.VMEM((half, patches, span), BF),
            pltpu.VMEM((half, 2, span, patches), BF),
            pltpu.VMEM((hidden, E), BF),
            pltpu.VMEM((slots, rows, E), BF),
            pltpu.VMEM((E, tokens), F32),
            pltpu.VMEM((2, patches, E), BF),
            pltpu.VMEM((2, patches, tokens), F32),
            pltpu.VMEM((2, patches, tokens), BF),
            pltpu.VMEM((slots, 1, tokens), F32),
            pltpu.VMEM((slots, rows, E), BF),
            pltpu.VMEM((slots, rows, E), BF),
            pltpu.VMEM((2, E, patches), BF),
            pltpu.VMEM((2, E, patches), BF),
            pltpu.VMEM((2, rows, E), BF),
            pltpu.VMEM((half, span, E), F32),
            pltpu.VMEM((slots, chunk, E), BF),
            pltpu.VMEM((slots, chunk, E), BF),
            dma(LOADS + 2 * len(KINDS)),
        ],
        compiler_params=pltpu.CompilerParams(
            collective_id=0, has_side_effects=True, vmem_limit_bytes=65536000
        ),
        name="fused",
    )(query_hidden, ph, projection, jnp.transpose(clicks, (0, 2, 1)), bins)
    query_grad, page_grad, weight_grad = pl.pallas_call(
        writer,
        out_shape=outs,
        in_specs=[vmem] * 3,
        out_specs=(hbm,) * 3,
        scratch_shapes=[dma(3)],
        compiler_params=pltpu.CompilerParams(vmem_limit_bytes=4 * 1024 * 1024),
        name="writer",
    )(*results)
    return query_grad, page_grad.reshape(page_hidden.shape), weight_grad


def solution(mesh):
    return jax.shard_map(
        functools.partial(shards, mesh.shape["pb"], mesh.shape["pa"]),
        mesh=mesh,
        in_specs=(
            P("pb", "pa", None),
            P("pa", "pb", None),
            P(),
            P("pb", None, None),
            P("pb", None),
        ),
        out_specs=(P("pb", "pa", None), P("pa", "pb", None), P(("pb", "pa"), None)),
        check_vma=False,
    )
```

```python
import functools
import math

import jax
import jax.numpy as jnp
from jax import lax
from jax.experimental import pallas as pl
from jax.experimental.pallas import tpu as pltpu
from jax.sharding import PartitionSpec as P

sharpness = 0.25
MESH = pl.DeviceIdType.MESH
BF = jnp.bfloat16
F32 = jnp.float32
FOLDED = sharpness * math.log2(math.e)
LOADS = 5
KINDS = ("query", "query_far", "click", "bin", "page", "hidden", "raw", "norm", "token", "patch", "low", "weight")


def dot(x, y, dims):
    return lax.dot_general(x, y, (dims, ((), ())), preferred_element_type=F32)


def kernel(
    PB, PA, qh_hbm, ph_hbm, proj_hbm, clicks_hbm, bins_hbm,
    qg_ref, pg_ref, w_ref,
    clicks_ref, bins_ref, qraw, qh, qb, qx, ph, hx, pht, proj, qe, qt, pe, lbuf, ebuf, ebt, tops, totals, norm,
    tsend, trecv, gsend, grecv, low, wq, wsend, wrecv, sems,
):
    b = lax.axis_index("pb")
    a = lax.axis_index("pa")
    queries, token_local, hidden = qh_hbm.shape
    rows = queries * token_local
    patches = ph_hbm.shape[0]
    E = proj.shape[1]
    half = PB // 2
    slots = half * PA
    tokens = slots * rows
    total_queries = half * queries
    parity = lax.rem(b, 2)
    level = b // 2
    me = level * PA + a
    partner = (b + 1 - 2 * parity, a)
    chunk = w_ref.shape[0]
    span = PA * chunk
    width = 2 if PA < 32 else 4
    deep = PA // width
    z = a // width
    x = lax.rem(a, width)
    upper = z >= deep // 2

    def sem(kind, receive):
        return sems.at[LOADS + 2 * KINDS.index(kind) + receive]

    def remote(kind, src, dst, to, received=None):
        c = pltpu.make_async_remote_copy(
            src_ref=src, dst_ref=dst, send_sem=sem(kind, 0), recv_sem=received or sem(kind, 1),
            device_id=to, device_id_type=MESH,
        )
        c.start()

    def drain(kind, ref, receive):
        pltpu.make_async_copy(ref, ref, sem(kind, receive)).wait()

    def others(offsets):
        for i in range(deep):
            far = jnp.where(upper, i, deep - 1 - i)
            for k in offsets:
                to_level = lax.rem(level + k, half)
                for j in list(range(1, width)) + [0]:
                    to_z = far
                    if k == 0 and j == 0:
                        if i == deep - 1:
                            continue
                        up = i + jnp.where(i >= z, 1, 0)
                        down = deep - 1 - i - jnp.where(deep - 1 - i <= z, 1, 0)
                        to_z = jnp.where(upper, up, down)
                    yield to_level, to_z * width + lax.rem(x + j, width)

    every = list(range(1, half)) + [0]

    def device(to_level, to_a):
        return 2 * to_level + parity, to_a

    barrier = pltpu.get_barrier_semaphore()
    for to in others(every):
        pl.semaphore_signal(barrier, inc=1, device_id=device(*to), device_id_type=MESH)
    pl.semaphore_signal(barrier, inc=1, device_id=partner, device_id_type=MESH)

    loads = [
        pltpu.make_async_copy(qh_hbm, qraw, sems.at[0]),
        pltpu.make_async_copy(proj_hbm, proj, sems.at[1]),
        pltpu.make_async_copy(ph_hbm, ph, sems.at[2]),
        pltpu.make_async_copy(clicks_hbm, clicks_ref.at[level], sems.at[3]),
        pltpu.make_async_copy(bins_hbm, bins_ref.at[level], sems.at[4]),
    ]
    for c in loads:
        c.start()
    loads[0].wait()
    for q in range(queries):
        qh[q * token_local:(q + 1) * token_local] = qraw[q].astype(F32)
    qb[...] = qh[...].astype(BF)
    loads[1].wait()
    qe[me] = dot(qb[...], proj[...], ((1,), (0,))).astype(BF)
    pl.semaphore_wait(barrier, slots)
    group = PA // 2
    side = a // group
    for to in others(every):
        other_side = jnp.where(to[1] // group == side, 0, 1)
        remote("query", qe.at[me], qe.at[me], device(*to), sems.at[LOADS + 1 + 2 * other_side])
    for k in range(1, half):
        to = device(lax.rem(level + k, half), a)
        remote("click", clicks_hbm, clicks_ref.at[level], to)
        remote("bin", bins_hbm, bins_ref.at[level], to)

    loads[2].wait()
    pe[0] = dot(ph[...], proj[...], ((1,), (0,))).astype(BF)
    remote("page", pe.at[0], pe.at[1], partner)

    def columns(l, core):
        return pl.ds(pl.multiple_of((2 * l + core) * span, 128), span)

    for l in range(half):
        remote("hidden", ph.at[:, columns(l, 1 - parity)], hx.at[l], partner)
        remote("raw", qb.at[:, columns(l, 1 - parity)], qx.at[l], partner)

    query_of = lax.broadcasted_iota(jnp.int32, (total_queries, tokens), 0)
    token_of = lax.broadcasted_iota(jnp.int32, (total_queries, tokens), 1)

    def belongs(query_id, token_id):
        own_query = lax.rem(token_id, rows) // token_local + token_id // (PA * rows) * queries
        return jnp.where(query_id == own_query, 1.0, 0.0)

    mask = belongs(query_of, token_of)
    for l in range(half):
        pht[l, 0] = ph[:, columns(l, parity)].T
    drain("hidden", hx, 1)
    for l in range(half):
        pht[l, 1] = hx[l].T

    drain("page", pe.at[0], 1)
    part_tokens = group * rows
    for near in (True, False):
        drain("query" if near else "query_far", qe.at[pl.ds(0, half * group - near)], 1)
        for l in range(half):
            start = l * PA + group * (side if near else 1 - side)
            lanes = pl.ds(pl.multiple_of(start * rows, 128), part_tokens)
            tok = qe[pl.ds(start, group)].reshape(part_tokens, E)
            top = None
            for k in range(2):
                block = dot(pe[k], tok, ((1,), (1,)))
                lbuf[k] = block
                high = jnp.max(block, axis=0, keepdims=True)
                top = high if top is None else jnp.maximum(top, high)
            total = None
            for k in range(2):
                e = jnp.exp2((lbuf[k] - top) * FOLDED)
                ebuf[k, :, lanes] = e.astype(BF)
                part = jnp.sum(e, axis=0, keepdims=True)
                total = part if total is None else total + part
            top = sharpness * top
            tops[:, lanes] = top
            totals[:, lanes] = total
            norm[me, :, lanes] = top + jnp.log(total)
    for to in others(every):
        remote("norm", norm.at[me], norm.at[me], device(*to))

    unit = dot(pe[0], ebuf[0], ((0,), (0,))) + dot(pe[1], ebuf[1], ((0,), (0,)))
    unit = (unit / totals[...]).T.astype(BF)
    for s in range(slots):
        tsend[s] = unit[s * rows:(s + 1) * rows]
    for to_level, to_a in others(every):
        remote("token", tsend.at[to_level * PA + to_a], trecv.at[me], device(to_level, to_a))
    trecv[me] = tsend[me]
    qt[...] = qe[...].reshape(tokens, E).astype(F32).T
    for k in range(2):
        ebt[k] = ebuf[k].T

    loads[3].wait()
    loads[4].wait()
    if half > 1:
        drain("click", clicks_ref.at[pl.ds(0, half - 1)], 1)
        drain("bin", bins_ref.at[pl.ds(0, half - 1)], 1)
    pairs = bins_ref.shape[2]
    pos = clicks_ref[:, :, 0, :].reshape(total_queries, pairs)
    neg = clicks_ref[:, :, 1, :].reshape(total_queries, pairs)
    weight = jnp.sqrt(bins_ref[...].reshape(total_queries, pairs).astype(F32) + 1.0)

    def merged(parts):
        high = functools.reduce(jnp.maximum, parts)
        return high + jnp.log(functools.reduce(jnp.add, [jnp.exp(v - high) for v in parts]))

    drain("norm", norm.at[pl.ds(0, slots - 1)], 1)
    at_pos = jnp.zeros(pos.shape, F32)
    at_neg = jnp.zeros(pos.shape, F32)
    rows_in = norm[...].reshape(slots, tokens)
    log_norms = merged([rows_in[l * PA:(l + 1) * PA] for l in range(half)])
    for p in range(PA):
        score = jnp.sum(mask * log_norms[p:p + 1], axis=1, keepdims=True)
        at_pos = at_pos + jnp.where(pos == p, score, 0.0)
        at_neg = at_neg + jnp.where(neg == p, score, 0.0)
    coeff = -weight * jax.nn.sigmoid(at_neg - at_pos)

    def score_grad(page):
        hits = (pos == page).astype(F32) - (neg == page).astype(F32)
        return jnp.sum(coeff * hits, axis=1, keepdims=True)

    log_norm = merged([norm[l * PA + a] for l in range(half)])
    factor = jnp.sum(mask * score_grad(a), axis=0, keepdims=True) * jnp.exp(tops[...] - log_norm)
    scaled = (qt[...] * factor).astype(BF)
    mine = []
    for k in range(2):
        part = dot(scaled, ebt[k], ((1,), (0,)))
        gsend[k] = part.astype(BF)
        remote("patch", gsend.at[k], grecv.at[k], partner)
        mine.append(part)

    lanes = min(128, tokens)
    first = me * rows // lanes * lanes
    near = pl.ds(pl.multiple_of(first, lanes), lanes)
    own_mask = belongs(
        lax.broadcasted_iota(jnp.int32, (total_queries, lanes), 0),
        first + lax.broadcasted_iota(jnp.int32, (total_queries, lanes), 1),
    )
    pick = jnp.where(
        lax.broadcasted_iota(jnp.int32, (rows, lanes), 0) + (me * rows - first)
        == lax.broadcasted_iota(jnp.int32, (rows, lanes), 1), 1.0, 0.0,
    )
    page_of = lax.broadcasted_iota(jnp.int32, (PA, lanes), 0)
    grads = jnp.zeros((PA, lanes), F32)
    for p in range(PA):
        grads = jnp.where(page_of == p, jnp.sum(own_mask * score_grad(p), axis=0, keepdims=True), grads)
    rows_in = norm[:, :, near].reshape(slots, lanes)
    parts = [rows_in[l * PA:(l + 1) * PA] for l in range(half)]
    log_norms = merged(parts)
    shares = []
    for l in range(half):
        factors = grads * jnp.exp(parts[l] - log_norms)
        for p in range(PA):
            shares.append(jnp.sum(pick * factors[p:p + 1], axis=1, keepdims=True))
    drain("token", trecv.at[pl.ds(0, slots - 1)], 1)
    token_own = None
    for s in range(slots):
        part = trecv[s].astype(F32) * shares[s]
        token_own = part if token_own is None else token_own + part
    token_low = (sharpness * token_own).astype(BF)
    low[0] = token_low
    remote("low", low.at[0], low.at[1], partner)

    drain("raw", qx, 1)
    drain("low", low.at[0], 1)
    for l in range(half):
        wq[l] = dot(qb[:, columns(l, parity)], token_low, ((0,), (0,))) + dot(qx[l], low[1], ((0,), (0,)))

    drain("patch", grecv, 1)
    patch_low = [(sharpness * (mine[k] + grecv[1 - k].astype(F32))).astype(BF).T for k in range(2)]

    for k in every:
        to_level = lax.rem(level + k, half)
        block = wq[to_level]
        for i in range(2):
            block = block + dot(pht[to_level, i], patch_low[i], ((1,), (0,)))
        block = block.astype(BF)
        for s in range(PA):
            wsend[to_level * PA + s] = block[s * chunk:(s + 1) * chunk]
    for to_level, to_a in others(every):
        remote("weight", wsend.at[to_level * PA + to_a], wrecv.at[me], device(to_level, to_a))
    wrecv[me] = wsend[me]

    qgrad = dot(token_low, proj[...], ((1,), (1,)))
    for q in range(queries):
        qg_ref[q] = qgrad[q * token_local:(q + 1) * token_local].astype(BF)
    pg_ref[...] = dot(patch_low[0], proj[...], ((1,), (1,))).astype(BF)

    drain("query", qe.at[pl.ds(0, slots - 1)], 0)
    if half > 1:
        drain("click", clicks_ref.at[pl.ds(0, half - 1)], 0)
        drain("bin", bins_ref.at[pl.ds(0, half - 1)], 0)
    drain("page", pe.at[0], 0)
    drain("hidden", hx, 0)
    drain("raw", qx, 0)
    drain("norm", norm.at[pl.ds(0, slots - 1)], 0)
    drain("token", tsend.at[pl.ds(0, slots - 1)], 0)
    drain("patch", gsend, 0)
    drain("low", low.at[0], 0)
    drain("weight", wsend.at[pl.ds(0, slots - 1)], 0)
    drain("weight", wrecv.at[pl.ds(0, slots - 1)], 1)
    weight_sum = wrecv[0].astype(F32)
    for s in range(1, slots):
        weight_sum = weight_sum + wrecv[s].astype(F32)
    w_ref[...] = weight_sum


def writer(qg, pg, w, qg_out, pg_out, w_out, sems):
    copies = [
        pltpu.make_async_copy(pg, pg_out, sems.at[0]),
        pltpu.make_async_copy(qg, qg_out, sems.at[1]),
        pltpu.make_async_copy(w, w_out, sems.at[2]),
    ]
    for c in copies:
        c.start()
    for c in copies:
        c.wait()


def shards(PB, PA, query_hidden, page_hidden, projection, clicks, bins):
    queries, token_local, hidden = query_hidden.shape
    page_count, patches, _ = page_hidden.shape
    assert page_count == 1 and PB % 2 == 0
    E = projection.shape[1]
    rows = queries * token_local
    half = PB // 2
    slots = half * PA
    tokens = rows * slots
    chunk = hidden // (PB * PA)
    span = PA * chunk
    pairs = clicks.shape[1]
    ph = page_hidden.reshape(patches, hidden)
    vmem = pl.BlockSpec(memory_space=pltpu.VMEM)
    hbm = pl.BlockSpec(memory_space=pltpu.HBM)
    dma = lambda n: pltpu.SemaphoreType.DMA((n,))
    outs = (
        jax.ShapeDtypeStruct(query_hidden.shape, BF),
        jax.ShapeDtypeStruct((patches, hidden), BF),
        jax.ShapeDtypeStruct((chunk, E), F32),
    )
    results = pl.pallas_call(
        functools.partial(kernel, PB, PA),
        out_shape=tuple(pltpu.VMEM(o.shape, o.dtype) for o in outs),
        in_specs=[hbm] * 5,
        out_specs=(vmem,) * 3,
        scratch_shapes=[
            pltpu.VMEM((half, queries, 2, pairs), jnp.int32),
            pltpu.VMEM((half, queries, pairs), jnp.int32),
            pltpu.VMEM(query_hidden.shape, BF),
            pltpu.VMEM((rows, hidden), F32),
            pltpu.VMEM((rows, hidden), BF),
            pltpu.VMEM((half, rows, span), BF),
            pltpu.VMEM((patches, hidden), BF),
            pltpu.VMEM((half, patches, span), BF),
            pltpu.VMEM((half, 2, span, patches), BF),
            pltpu.VMEM((hidden, E), BF),
            pltpu.VMEM((slots, rows, E), BF),
            pltpu.VMEM((E, tokens), F32),
            pltpu.VMEM((2, patches, E), BF),
            pltpu.VMEM((2, patches, tokens // half // 2), F32),
            pltpu.VMEM((2, patches, tokens), BF),
            pltpu.VMEM((2, tokens, patches), BF),
            pltpu.VMEM((1, tokens), F32),
            pltpu.VMEM((1, tokens), F32),
            pltpu.VMEM((slots, 1, tokens), F32),
            pltpu.VMEM((slots, rows, E), BF),
            pltpu.VMEM((slots, rows, E), BF),
            pltpu.VMEM((2, E, patches), BF),
            pltpu.VMEM((2, E, patches), BF),
            pltpu.VMEM((2, rows, E), BF),
            pltpu.VMEM((half, span, E), F32),
            pltpu.VMEM((slots, chunk, E), BF),
            pltpu.VMEM((slots, chunk, E), BF),
            dma(LOADS + 2 * len(KINDS)),
        ],
        compiler_params=pltpu.CompilerParams(
            collective_id=0, has_side_effects=True, vmem_limit_bytes=65536000
        ),
        name="fused",
    )(query_hidden, ph, projection, jnp.transpose(clicks, (0, 2, 1)), bins)
    query_grad, page_grad, weight_grad = pl.pallas_call(
        writer,
        out_shape=outs,
        in_specs=[vmem] * 3,
        out_specs=(hbm,) * 3,
        scratch_shapes=[dma(3)],
        compiler_params=pltpu.CompilerParams(vmem_limit_bytes=4 * 1024 * 1024),
        name="writer",
    )(*results)
    return query_grad, page_grad.reshape(page_hidden.shape), weight_grad


def solution(mesh):
    return jax.shard_map(
        functools.partial(shards, mesh.shape["pb"], mesh.shape["pa"]),
        mesh=mesh,
        in_specs=(
            P("pb", "pa", None),
            P("pa", "pb", None),
            P(),
            P("pb", None, None),
            P("pb", None),
        ),
        out_specs=(P("pb", "pa", None), P("pa", "pb", None), P(("pb", "pa"), None)),
        check_vma=False,
    )
```

```python
import functools
import math

import jax
import jax.numpy as jnp
from jax import lax
from jax.experimental import pallas as pl
from jax.experimental.pallas import tpu as pltpu
from jax.sharding import PartitionSpec as P

sharpness = 0.25
MESH = pl.DeviceIdType.MESH
BF = jnp.bfloat16
F32 = jnp.float32
FOLDED = sharpness * math.log2(math.e)
RECEIVED = (
    "near", "far", "click", "bin", "page", "other", "hidden", "raw", "level", "norm", "token", "patch", "low", "weight",
)
LOADS = 5


def dot(x, y, dims):
    return lax.dot_general(x, y, (dims, ((), ())), preferred_element_type=F32)


def kernel(
    PB, PA, qh_hbm, ph_hbm, proj_hbm, clicks_hbm, bins_hbm,
    qg_ref, pg_ref, w_ref,
    clicks_ref, bins_ref, qraw, qh, qb, qx, ph, hx, pht, proj, qe, qt, pe, po, lbuf, ebuf, ebt, eo, tops, sums, norm,
    tsend, trecv, gsend, grecv, low, wq, wsend, wrecv, arrived,
):
    b = lax.axis_index("pb")
    a = lax.axis_index("pa")
    queries, token_local, hidden = qh_hbm.shape
    rows = queries * token_local
    patches = ph_hbm.shape[0]
    E = proj.shape[1]
    half = PB // 2
    slots = half * PA
    level_tokens = PA * rows
    tokens = half * level_tokens
    parity = lax.rem(b, 2)
    level = b // 2
    me = level * PA + a
    partner = (b + 1 - 2 * parity, a)
    chunk = w_ref.shape[0]
    span = PA * chunk
    width = 2 if PA < 32 else 4
    deep = PA // width
    z = a // width
    x = lax.rem(a, width)
    upper = z >= deep // 2
    group = PA // 2
    side = a // group

    def others(offsets):
        for i in range(deep):
            far = jnp.where(upper, i, deep - 1 - i)
            for k in offsets:
                to_level = lax.rem(level + k, half)
                for j in list(range(1, width)) + [0]:
                    to_z = far
                    if k == 0 and j == 0:
                        if i == deep - 1:
                            continue
                        up = i + jnp.where(i >= z, 1, 0)
                        down = deep - 1 - i - jnp.where(deep - 1 - i <= z, 1, 0)
                        to_z = jnp.where(upper, up, down)
                    yield to_level, to_z * width + lax.rem(x + j, width)

    every = list(range(1, half)) + [0]

    def device(to_level, to_a):
        return 2 * to_level + parity, to_a

    def across(k):
        to_level = lax.rem(level + k, half)
        return device(to_level, a), (2 * to_level + 1 - parity, a)

    barrier = pltpu.get_barrier_semaphore()
    for to in others([0]):
        pl.semaphore_signal(barrier, inc=1, device_id=device(*to), device_id_type=MESH)
    for k in range(1, half):
        for to in across(k):
            pl.semaphore_signal(barrier, inc=1, device_id=to, device_id_type=MESH)
    pl.semaphore_signal(barrier, inc=1, device_id=partner, device_id_type=MESH)

    def body(sent):
        def remote(kind, src, dst, to, received=None):
            pltpu.make_async_remote_copy(
                src_ref=src, dst_ref=dst, send_sem=sent.at[LOADS + RECEIVED.index(kind)],
                recv_sem=arrived.at[RECEIVED.index(kind)] if received is None else received,
                device_id=to, device_id_type=MESH,
            ).start()

        def receive(kind, ref):
            pltpu.make_async_copy(ref, ref, arrived.at[RECEIVED.index(kind)]).wait()

        def flush(kind, ref):
            pltpu.make_async_copy(ref, ref, sent.at[LOADS + RECEIVED.index(kind)]).wait()

        loads = [
            pltpu.make_async_copy(qh_hbm, qraw, sent.at[0]),
            pltpu.make_async_copy(proj_hbm, proj, sent.at[1]),
            pltpu.make_async_copy(ph_hbm, ph, sent.at[2]),
            pltpu.make_async_copy(clicks_hbm, clicks_ref.at[level], sent.at[3]),
            pltpu.make_async_copy(bins_hbm, bins_ref.at[level], sent.at[4]),
        ]
        for c in loads:
            c.start()
        loads[0].wait()
        for q in range(queries):
            qh[q * token_local:(q + 1) * token_local] = qraw[q].astype(F32)
        qb[...] = qh[...].astype(BF)
        loads[1].wait()
        qe[me] = dot(qb[...], proj[...], ((1,), (0,))).astype(BF)
        loads[2].wait()
        pe[0] = dot(ph[...], proj[...], ((1,), (0,))).astype(BF)
        pl.semaphore_wait(barrier, PA + 2 * (half - 1))
        for to in others([0]):
            other_side = jnp.where(to[1] // group == side, 0, 1)
            remote("near", qe.at[me], qe.at[me], device(*to), arrived.at[other_side])
        for k in range(1, half):
            for to in across(k):
                remote("other", pe.at[0], po.at[k - 1, parity], to)
        remote("page", pe.at[0], pe.at[1], partner)
        for k in range(1, half):
            to = across(k)[0]
            remote("click", clicks_hbm, clicks_ref.at[level], to)
            remote("bin", bins_hbm, bins_ref.at[level], to)

        def columns(l, core):
            return pl.ds(pl.multiple_of((2 * l + core) * span, 128), span)

        for l in range(half):
            remote("hidden", ph.at[:, columns(l, 1 - parity)], hx.at[l], partner)
            remote("raw", qb.at[:, columns(l, 1 - parity)], qx.at[l], partner)

        query_of = lax.broadcasted_iota(jnp.int32, (queries, level_tokens), 0)
        token_of = lax.broadcasted_iota(jnp.int32, (queries, level_tokens), 1)
        mask = jnp.where(query_of == lax.rem(token_of, rows) // token_local, 1.0, 0.0)
        for l in range(half):
            pht[l, 0] = ph[:, columns(l, parity)].T
        receive("hidden", hx)
        for l in range(half):
            pht[l, 1] = hx[l].T

        def spread(pages, tok, store):
            top = None
            count = tok.shape[0]
            for k in range(2):
                block = dot(pages(k), tok, ((1,), (1,)))
                lbuf[k, :, :count] = block
                high = jnp.max(block, axis=0, keepdims=True)
                top = high if top is None else jnp.maximum(top, high)
            total = None
            for k in range(2):
                e = jnp.exp2((lbuf[k, :, :count] - top) * FOLDED)
                store(k, e.astype(BF))
                part = jnp.sum(e, axis=0, keepdims=True)
                total = part if total is None else total + part
            return sharpness * top, total

        def lanes_of(start, count):
            return pl.ds(pl.multiple_of(start * rows, 128), count * rows)

        def own_chip(start, count):
            lanes = lanes_of(start, count)

            def store(k, e):
                ebuf[k, :, lanes] = e

            tok = qe[pl.ds(start, count)].reshape(count * rows, E)
            tops[:, lanes], sums[:, lanes] = spread(lambda k: pe[k], tok, store)

        receive("page", pe.at[0])
        receive("near", qe.at[pl.ds(0, group - 1)])
        own_chip(level * PA + group * side, group)
        receive("far", qe.at[pl.ds(0, group)])
        own_chip(level * PA + group * (1 - side), group)
        here = lanes_of(level * PA, PA)
        highs, totals = [tops[:, here]], [sums[:, here]]
        if half > 1:
            receive("other", po)
        for g in range(half - 1):
            def store(k, e):
                eo[g, k] = e

            tok = qe[pl.ds(level * PA, PA)].reshape(level_tokens, E)
            high, total = spread(lambda k: po[g, k], tok, store)
            highs.append(high)
            totals.append(total)
        high = functools.reduce(jnp.maximum, highs)
        total = functools.reduce(jnp.add, [t * jnp.exp(h - high) for h, t in zip(highs, totals)])
        log_norm = high + jnp.log(total)
        norm[me] = log_norm
        for to in others(every):
            remote("norm", norm.at[me], norm.at[me], device(*to))
        for k in range(1, half):
            mine = qe.at[pl.ds(level * PA, PA)]
            remote("level", mine, mine, across(k)[0])

        unit = None
        for g in range(half):
            for k in range(2):
                if g:
                    part = dot(po[g - 1, k], eo[g - 1, k], ((0,), (0,)))
                else:
                    part = dot(pe[k], ebuf[k, :, here], ((0,), (0,)))
                part = part * jnp.exp(highs[g] - log_norm)
                unit = part if unit is None else unit + part
        unit = unit.T.astype(BF)
        for s in range(PA):
            tsend[s] = unit[s * rows:(s + 1) * rows]
        for to_level, to_a in others([0]):
            remote("token", tsend.at[to_a], trecv.at[a], device(to_level, to_a))
        trecv[a] = tsend[a]
        for k in range(2):
            ebt[k, lanes_of(level * PA, PA)] = ebuf[k, :, here].T
        if half > 1:
            receive("level", qe.at[pl.ds(0, (half - 1) * PA)])
        for g in range(1, half):
            start = lax.rem(level + g, half) * PA
            own_chip(start, PA)
            for k in range(2):
                ebt[k, lanes_of(start, PA)] = ebuf[k, :, lanes_of(start, PA)].T
        qt[...] = qe[...].reshape(tokens, E).astype(F32).T

        loads[3].wait()
        loads[4].wait()
        if half > 1:
            receive("click", clicks_ref.at[pl.ds(0, half - 1)])
            receive("bin", bins_ref.at[pl.ds(0, half - 1)])
        pos = [clicks_ref[l, :, 0, :] for l in range(half)]
        neg = [clicks_ref[l, :, 1, :] for l in range(half)]
        weight = [jnp.sqrt(bins_ref[l].astype(F32) + 1.0) for l in range(half)]

        receive("norm", norm.at[pl.ds(0, slots - 1)])
        coeff = []
        for l in range(half):
            rows_in = norm[l * PA:(l + 1) * PA].reshape(PA, level_tokens)
            gap = jnp.zeros(pos[l].shape, F32)
            away = jnp.zeros(pos[l].shape, F32)
            for p in range(PA):
                score = jnp.sum(mask * rows_in[p:p + 1], axis=1, keepdims=True)
                gap = gap + jnp.where(pos[l] == p, score, 0.0)
                away = away + jnp.where(neg[l] == p, score, 0.0)
            coeff.append(-weight[l] * jax.nn.sigmoid(away - gap))

        def score_grad(l, page):
            hits = (pos[l] == page).astype(F32) - (neg[l] == page).astype(F32)
            return jnp.sum(coeff[l] * hits, axis=1, keepdims=True)

        scaled = []
        for l in range(half):
            at = slice(l * level_tokens, (l + 1) * level_tokens)
            factor = jnp.sum(mask * score_grad(l, a), axis=0, keepdims=True)
            factor = factor * jnp.exp(tops[:, at] - norm[l * PA + a])
            scaled.append((qt[:, at] * factor).astype(BF))
        scaled = jnp.concatenate(scaled, axis=1)
        mine = []
        for k in range(2):
            part = dot(scaled, ebt[k], ((1,), (0,)))
            gsend[k] = part.astype(BF)
            remote("patch", gsend.at[k], grecv.at[k], partner)
            mine.append(part)

        column = lax.broadcasted_iota(jnp.int32, (queries, 128), 1)
        table = jnp.zeros((queries, 128), F32)
        for p in range(PA):
            grad = jnp.zeros((queries, 1), F32)
            for l in range(half):
                grad = grad + jnp.where(level == l, score_grad(l, p), 0.0)
            table = jnp.where(column == p, grad, table)
        row_of = lax.broadcasted_iota(jnp.int32, (rows, 128), 0) // token_local
        shares = jnp.zeros((rows, 128), F32)
        for q in range(queries):
            shares = jnp.where(row_of == q, table[q:q + 1], shares)
        receive("token", trecv.at[pl.ds(0, PA - 1)])
        token_own = None
        for p in range(PA):
            part = trecv[p].astype(F32) * shares[:, p:p + 1]
            token_own = part if token_own is None else token_own + part
        token_low = (sharpness * token_own).astype(BF)
        low[0] = token_low
        remote("low", low.at[0], low.at[1], partner)

        receive("raw", qx)
        receive("low", low.at[0])
        for l in range(half):
            wq[l] = dot(qb[:, columns(l, parity)], token_low, ((0,), (0,))) + dot(qx[l], low[1], ((0,), (0,)))

        receive("patch", grecv)
        patch_low = [(sharpness * (mine[k] + grecv[1 - k].astype(F32))).astype(BF).T for k in range(2)]

        for k in every:
            to_level = lax.rem(level + k, half)
            block = wq[to_level]
            for i in range(2):
                block = block + dot(pht[to_level, i], patch_low[i], ((1,), (0,)))
            block = block.astype(BF)
            for s in range(PA):
                wsend[to_level * PA + s] = block[s * chunk:(s + 1) * chunk]
        for to_level, to_a in others(every):
            remote("weight", wsend.at[to_level * PA + to_a], wrecv.at[me], device(to_level, to_a))
        wrecv[me] = wsend[me]

        qgrad = dot(token_low, proj[...], ((1,), (1,)))
        for q in range(queries):
            qg_ref[q] = qgrad[q * token_local:(q + 1) * token_local].astype(BF)
        pg_ref[...] = dot(patch_low[0], proj[...], ((1,), (1,))).astype(BF)

        flush("near", qe.at[pl.ds(0, PA - 1)])
        if half > 1:
            flush("click", clicks_ref.at[pl.ds(0, half - 1)])
            flush("bin", bins_ref.at[pl.ds(0, half - 1)])
            flush("other", po)
            flush("level", qe.at[pl.ds(0, (half - 1) * PA)])
        flush("page", pe.at[0])
        flush("hidden", hx)
        flush("raw", qx)
        flush("norm", norm.at[pl.ds(0, slots - 1)])
        flush("token", tsend.at[pl.ds(0, PA - 1)])
        flush("patch", gsend)
        flush("low", low.at[0])
        flush("weight", wsend.at[pl.ds(0, slots - 1)])
        receive("weight", wrecv.at[pl.ds(0, slots - 1)])
        weight_sum = wrecv[0].astype(F32)
        for s in range(1, slots):
            weight_sum = weight_sum + wrecv[s].astype(F32)
        w_ref[...] = weight_sum

    pl.run_scoped(body, pltpu.SemaphoreType.DMA((LOADS + len(RECEIVED),)))


def writer(qg, pg, w, qg_out, pg_out, w_out, sems):
    copies = [
        pltpu.make_async_copy(pg, pg_out, sems.at[0]),
        pltpu.make_async_copy(qg, qg_out, sems.at[1]),
        pltpu.make_async_copy(w, w_out, sems.at[2]),
    ]
    for c in copies:
        c.start()
    for c in copies:
        c.wait()


def shards(PB, PA, query_hidden, page_hidden, projection, clicks, bins):
    queries, token_local, hidden = query_hidden.shape
    page_count, patches, _ = page_hidden.shape
    assert page_count == 1 and PB % 2 == 0
    E = projection.shape[1]
    rows = queries * token_local
    half = PB // 2
    slots = half * PA
    tokens = rows * slots
    chunk = hidden // (PB * PA)
    span = PA * chunk
    pairs = clicks.shape[1]
    ph = page_hidden.reshape(patches, hidden)
    vmem = pl.BlockSpec(memory_space=pltpu.VMEM)
    hbm = pl.BlockSpec(memory_space=pltpu.HBM)
    dma = lambda n: pltpu.SemaphoreType.DMA((n,))
    outs = (
        jax.ShapeDtypeStruct(query_hidden.shape, BF),
        jax.ShapeDtypeStruct((patches, hidden), BF),
        jax.ShapeDtypeStruct((chunk, E), F32),
    )
    results = pl.pallas_call(
        functools.partial(kernel, PB, PA),
        out_shape=tuple(pltpu.VMEM(o.shape, o.dtype) for o in outs),
        in_specs=[hbm] * 5,
        out_specs=(vmem,) * 3,
        scratch_shapes=[
            pltpu.VMEM((half, queries, 2, pairs), jnp.int32),
            pltpu.VMEM((half, queries, pairs), jnp.int32),
            pltpu.VMEM(query_hidden.shape, BF),
            pltpu.VMEM((rows, hidden), F32),
            pltpu.VMEM((rows, hidden), BF),
            pltpu.VMEM((half, rows, span), BF),
            pltpu.VMEM((patches, hidden), BF),
            pltpu.VMEM((half, patches, span), BF),
            pltpu.VMEM((half, 2, span, patches), BF),
            pltpu.VMEM((hidden, E), BF),
            pltpu.VMEM((slots, rows, E), BF),
            pltpu.VMEM((E, tokens), F32),
            pltpu.VMEM((2, patches, E), BF),
            pltpu.VMEM((max(half - 1, 1), 2, patches, E), BF),
            pltpu.VMEM((2, patches, PA * rows), F32),
            pltpu.VMEM((2, patches, tokens), BF),
            pltpu.VMEM((2, tokens, patches), BF),
            pltpu.VMEM((max(half - 1, 1), 2, patches, PA * rows), BF),
            pltpu.VMEM((1, tokens), F32),
            pltpu.VMEM((1, tokens), F32),
            pltpu.VMEM((slots, 1, PA * rows), F32),
            pltpu.VMEM((PA, rows, E), BF),
            pltpu.VMEM((PA, rows, E), BF),
            pltpu.VMEM((2, E, patches), BF),
            pltpu.VMEM((2, E, patches), BF),
            pltpu.VMEM((2, rows, E), BF),
            pltpu.VMEM((half, span, E), F32),
            pltpu.VMEM((slots, chunk, E), BF),
            pltpu.VMEM((slots, chunk, E), BF),
            dma(len(RECEIVED)),
        ],
        compiler_params=pltpu.CompilerParams(
            collective_id=0, has_side_effects=True, vmem_limit_bytes=65536000
        ),
        name="fused",
    )(query_hidden, ph, projection, jnp.transpose(clicks, (0, 2, 1)), bins)
    query_grad, page_grad, weight_grad = pl.pallas_call(
        writer,
        out_shape=outs,
        in_specs=[vmem] * 3,
        out_specs=(hbm,) * 3,
        scratch_shapes=[dma(3)],
        compiler_params=pltpu.CompilerParams(vmem_limit_bytes=4 * 1024 * 1024),
        name="writer",
    )(*results)
    return query_grad, page_grad.reshape(page_hidden.shape), weight_grad


def solution(mesh):
    return jax.shard_map(
        functools.partial(shards, mesh.shape["pb"], mesh.shape["pa"]),
        mesh=mesh,
        in_specs=(
            P("pb", "pa", None),
            P("pa", "pb", None),
            P(),
            P("pb", None, None),
            P("pb", None),
        ),
        out_specs=(P("pb", "pa", None), P("pa", "pb", None), P(("pb", "pa"), None)),
        check_vma=False,
    )
```

```python
import functools
import math

import jax
import jax.numpy as jnp
from jax import lax
from jax.experimental import pallas as pl
from jax.experimental.pallas import tpu as pltpu
from jax.sharding import PartitionSpec as P

sharpness = 0.25
MESH = pl.DeviceIdType.MESH
BF = jnp.bfloat16
F32 = jnp.float32
FOLDED = sharpness * math.log2(math.e)
RECEIVED = (
    "near", "far", "click", "bin", "page", "other", "hidden", "raw", "level", "norm", "token", "patch", "low", "weight",
)
LOADS = 5


def dot(x, y, dims):
    return lax.dot_general(x, y, (dims, ((), ())), preferred_element_type=F32)


def kernel(
    PB, PA, qh_hbm, ph_hbm, proj_hbm, clicks_hbm, bins_hbm,
    qg_ref, pg_ref, w_ref,
    clicks_ref, bins_ref, qraw, qh, qb, qx, qt2, ph, hx, pht, proj, qe, qt, pe, po, lbuf, ebuf, ebt, eo, tops, sums, norm,
    tsend, trecv, gsend, grecv, low, wq, wsend, wrecv, arrived,
):
    b = lax.axis_index("pb")
    a = lax.axis_index("pa")
    queries, token_local, hidden = qh_hbm.shape
    rows = queries * token_local
    patches = ph_hbm.shape[0]
    E = proj.shape[1]
    half = PB // 2
    slots = half * PA
    level_tokens = PA * rows
    tokens = half * level_tokens
    parity = lax.rem(b, 2)
    level = b // 2
    me = level * PA + a
    partner = (b + 1 - 2 * parity, a)
    chunk = w_ref.shape[0]
    span = PA * chunk
    width = 2 if PA < 32 else 4
    deep = PA // width
    z = a // width
    x = lax.rem(a, width)
    upper = z >= deep // 2
    group = PA // 2
    side = a // group

    def others(offsets, ascending=False):
        for i in range(deep):
            far = i if ascending else jnp.where(upper, i, deep - 1 - i)
            for k in offsets:
                to_level = lax.rem(level + k, half)
                for j in list(range(1, width)) + [0]:
                    to_z = far
                    if k == 0 and j == 0:
                        if i == deep - 1:
                            continue
                        up = i + jnp.where(i >= z, 1, 0)
                        down = deep - 1 - i - jnp.where(deep - 1 - i <= z, 1, 0)
                        to_z = up if ascending else jnp.where(upper, up, down)
                    yield to_level, to_z * width + lax.rem(x + j, width)

    every = list(range(1, half)) + [0]

    def device(to_level, to_a):
        return 2 * to_level + parity, to_a

    def across(k):
        to_level = lax.rem(level + k, half)
        return device(to_level, a), (2 * to_level + 1 - parity, a)

    barrier = pltpu.get_barrier_semaphore()
    for to in others([0]):
        pl.semaphore_signal(barrier, inc=1, device_id=device(*to), device_id_type=MESH)
    for k in range(1, half):
        for to in across(k):
            pl.semaphore_signal(barrier, inc=1, device_id=to, device_id_type=MESH)
    pl.semaphore_signal(barrier, inc=1, device_id=partner, device_id_type=MESH)

    def body(sent):
        def remote(kind, src, dst, to, received=None):
            pltpu.make_async_remote_copy(
                src_ref=src, dst_ref=dst, send_sem=sent.at[LOADS + RECEIVED.index(kind)],
                recv_sem=arrived.at[RECEIVED.index(kind)] if received is None else received,
                device_id=to, device_id_type=MESH,
            ).start()

        def receive(kind, ref):
            pltpu.make_async_copy(ref, ref, arrived.at[RECEIVED.index(kind)]).wait()

        def flush(kind, ref):
            pltpu.make_async_copy(ref, ref, sent.at[LOADS + RECEIVED.index(kind)]).wait()

        loads = [
            pltpu.make_async_copy(qh_hbm, qraw, sent.at[0]),
            pltpu.make_async_copy(proj_hbm, proj, sent.at[1]),
            pltpu.make_async_copy(ph_hbm, ph, sent.at[2]),
            pltpu.make_async_copy(clicks_hbm, clicks_ref.at[level], sent.at[3]),
            pltpu.make_async_copy(bins_hbm, bins_ref.at[level], sent.at[4]),
        ]
        for c in loads:
            c.start()
        loads[0].wait()
        for q in range(queries):
            qh[q * token_local:(q + 1) * token_local] = qraw[q].astype(F32)
        qb[...] = qh[...].astype(BF)
        loads[1].wait()
        qe[me] = dot(qb[...], proj[...], ((1,), (0,))).astype(BF)
        loads[2].wait()
        pe[0] = dot(ph[...], proj[...], ((1,), (0,))).astype(BF)
        pl.semaphore_wait(barrier, PA + 2 * (half - 1))
        for k in range(1, half):
            for to in across(k):
                remote("other", pe.at[0], po.at[k - 1, parity], to)
        for to in others([0]):
            other_side = jnp.where(to[1] // group == side, 0, 1)
            remote("near", qe.at[me], qe.at[me], device(*to), arrived.at[other_side])
        remote("page", pe.at[0], pe.at[1], partner)
        for k in range(1, half):
            to = across(k)[0]
            remote("click", clicks_hbm, clicks_ref.at[level], to)
            remote("bin", bins_hbm, bins_ref.at[level], to)

        def columns(l, core):
            return pl.ds(pl.multiple_of((2 * l + core) * span, 128), span)

        for l in range(half):
            remote("hidden", ph.at[:, columns(l, 1 - parity)], hx.at[l], partner)
            remote("raw", qb.at[:, columns(l, 1 - parity)], qx.at[l], partner)

        query_of = lax.broadcasted_iota(jnp.int32, (queries, level_tokens), 0)
        token_of = lax.broadcasted_iota(jnp.int32, (queries, level_tokens), 1)
        mask = jnp.where(query_of == lax.rem(token_of, rows) // token_local, 1.0, 0.0)
        for l in range(half):
            pht[l, 0] = ph[:, columns(l, parity)].T
        receive("hidden", hx)
        for l in range(half):
            pht[l, 1] = hx[l].T
        receive("raw", qx)
        for l in range(half):
            qt2[l, :, :rows] = qb[:, columns(l, parity)].T
            qt2[l, :, rows:] = qx[l].T

        def spread(pages, tok, store):
            top = None
            count = tok.shape[0]
            for k in range(2):
                block = dot(pages(k), tok, ((1,), (1,)))
                lbuf[k, :, :count] = block
                high = jnp.max(block, axis=0, keepdims=True)
                top = high if top is None else jnp.maximum(top, high)
            total = None
            for k in range(2):
                e = jnp.exp2((lbuf[k, :, :count] - top) * FOLDED)
                store(k, e.astype(BF))
                part = jnp.sum(e, axis=0, keepdims=True)
                total = part if total is None else total + part
            return sharpness * top, total

        def lanes_of(start, count):
            return pl.ds(pl.multiple_of(start * rows, 128), count * rows)

        def own_chip(start, count):
            lanes = lanes_of(start, count)

            def store(k, e):
                ebuf[k, :, lanes] = e

            tok = qe[pl.ds(start, count)].reshape(count * rows, E)
            tops[:, lanes], sums[:, lanes] = spread(lambda k: pe[k], tok, store)

        receive("page", pe.at[0])
        receive("near", qe.at[pl.ds(0, group - 1)])
        own_chip(level * PA + group * side, group)
        receive("far", qe.at[pl.ds(0, group)])
        own_chip(level * PA + group * (1 - side), group)
        here = lanes_of(level * PA, PA)
        highs, totals = [tops[:, here]], [sums[:, here]]
        if half > 1:
            receive("other", po)
        for g in range(half - 1):
            def store(k, e):
                eo[g, k] = e

            tok = qe[pl.ds(level * PA, PA)].reshape(level_tokens, E)
            high, total = spread(lambda k: po[g, k], tok, store)
            highs.append(high)
            totals.append(total)
        high = functools.reduce(jnp.maximum, highs)
        total = functools.reduce(jnp.add, [t * jnp.exp(h - high) for h, t in zip(highs, totals)])
        log_norm = high + jnp.log(total)
        norm[me] = log_norm
        for to in others(every):
            remote("norm", norm.at[me], norm.at[me], device(*to))
        for k in range(1, half):
            mine = qe.at[pl.ds(level * PA, PA)]
            remote("level", mine, mine, across(k)[0])

        unit = None
        for g in range(half):
            for k in range(2):
                if g:
                    part = dot(po[g - 1, k], eo[g - 1, k], ((0,), (0,)))
                else:
                    part = dot(pe[k], ebuf[k, :, here], ((0,), (0,)))
                part = part * jnp.exp(highs[g] - log_norm)
                unit = part if unit is None else unit + part
        unit = unit.T.astype(BF)
        for s in range(PA):
            tsend[s] = unit[s * rows:(s + 1) * rows]
        for to_level, to_a in others([0]):
            remote("token", tsend.at[to_a], trecv.at[a], device(to_level, to_a))
        trecv[a] = tsend[a]
        for k in range(2):
            ebt[k, lanes_of(level * PA, PA)] = ebuf[k, :, here].T
        if half > 1:
            receive("level", qe.at[pl.ds(0, (half - 1) * PA)])
        for g in range(1, half):
            start = lax.rem(level + g, half) * PA
            own_chip(start, PA)
            for k in range(2):
                ebt[k, lanes_of(start, PA)] = ebuf[k, :, lanes_of(start, PA)].T
        qt[...] = qe[...].reshape(tokens, E).astype(F32).T

        loads[3].wait()
        loads[4].wait()
        if half > 1:
            receive("click", clicks_ref.at[pl.ds(0, half - 1)])
            receive("bin", bins_ref.at[pl.ds(0, half - 1)])
        pos = [clicks_ref[l, :, 0, :] for l in range(half)]
        neg = [clicks_ref[l, :, 1, :] for l in range(half)]
        weight = [jnp.sqrt(bins_ref[l].astype(F32) + 1.0) for l in range(half)]

        receive("norm", norm.at[pl.ds(0, slots - 1)])
        coeff = []
        for l in range(half):
            rows_in = norm[l * PA:(l + 1) * PA].reshape(PA, level_tokens)
            gap = jnp.zeros(pos[l].shape, F32)
            away = jnp.zeros(pos[l].shape, F32)
            for p in range(PA):
                score = jnp.sum(mask * rows_in[p:p + 1], axis=1, keepdims=True)
                gap = gap + jnp.where(pos[l] == p, score, 0.0)
                away = away + jnp.where(neg[l] == p, score, 0.0)
            coeff.append(-weight[l] * jax.nn.sigmoid(away - gap))

        def score_grad(l, page):
            hits = (pos[l] == page).astype(F32) - (neg[l] == page).astype(F32)
            return jnp.sum(coeff[l] * hits, axis=1, keepdims=True)

        scaled = []
        for l in range(half):
            at = slice(l * level_tokens, (l + 1) * level_tokens)
            factor = jnp.sum(mask * score_grad(l, a), axis=0, keepdims=True)
            factor = factor * jnp.exp(tops[:, at] - norm[l * PA + a])
            scaled.append((qt[:, at] * factor).astype(BF))
        scaled = jnp.concatenate(scaled, axis=1)
        mine = []
        for k in range(2):
            part = dot(scaled, ebt[k], ((1,), (0,)))
            gsend[k] = part.astype(BF)
            remote("patch", gsend.at[k], grecv.at[k], partner)
            mine.append(part)

        column = lax.broadcasted_iota(jnp.int32, (queries, 128), 1)
        table = jnp.zeros((queries, 128), F32)
        for p in range(PA):
            grad = jnp.zeros((queries, 1), F32)
            for l in range(half):
                grad = grad + jnp.where(level == l, score_grad(l, p), 0.0)
            table = jnp.where(column == p, grad, table)
        row_of = lax.broadcasted_iota(jnp.int32, (rows, 128), 0) // token_local
        shares = jnp.zeros((rows, 128), F32)
        for q in range(queries):
            shares = jnp.where(row_of == q, table[q:q + 1], shares)
        receive("token", trecv.at[pl.ds(0, PA - 1)])
        token_own = None
        for p in range(PA):
            part = trecv[p].astype(F32) * shares[:, p:p + 1]
            token_own = part if token_own is None else token_own + part
        token_low = (sharpness * token_own).astype(BF)
        low[0] = token_low
        remote("low", low.at[0], low.at[1], partner)

        receive("low", low.at[0])
        for l in range(half):
            wq[l] = dot(qt2[l], low[...].reshape(2 * rows, E), ((1,), (0,)))

        receive("patch", grecv)
        patch_low = [(sharpness * (mine[k] + grecv[1 - k].astype(F32))).astype(BF).T for k in range(2)]

        for k in every:
            to_level = lax.rem(level + k, half)
            block = wq[to_level]
            for i in range(2):
                block = block + dot(pht[to_level, i], patch_low[i], ((1,), (0,)))
            block = block.astype(BF)
            for s in range(PA):
                wsend[to_level * PA + s] = block[s * chunk:(s + 1) * chunk]
        place = a * half + level
        for n in range(slots - 1):
            d = n + jnp.where(n >= place, 1, 0)
            to_level, to_a = lax.rem(d, half), d // half
            remote("weight", wsend.at[to_level * PA + to_a], wrecv.at[me], device(to_level, to_a))
        wrecv[me] = wsend[me]

        qgrad = dot(token_low, proj[...], ((1,), (1,)))
        for q in range(queries):
            qg_ref[q] = qgrad[q * token_local:(q + 1) * token_local].astype(BF)
        pg_ref[...] = dot(patch_low[0], proj[...], ((1,), (1,))).astype(BF)

        flush("near", qe.at[pl.ds(0, PA - 1)])
        if half > 1:
            flush("click", clicks_ref.at[pl.ds(0, half - 1)])
            flush("bin", bins_ref.at[pl.ds(0, half - 1)])
            flush("other", po)
            flush("level", qe.at[pl.ds(0, (half - 1) * PA)])
        flush("page", pe.at[0])
        flush("hidden", hx)
        flush("raw", qx)
        flush("norm", norm.at[pl.ds(0, slots - 1)])
        flush("token", tsend.at[pl.ds(0, PA - 1)])
        flush("patch", gsend)
        flush("low", low.at[0])
        flush("weight", wsend.at[pl.ds(0, slots - 1)])
        receive("weight", wrecv.at[pl.ds(0, slots - 1)])
        weight_sum = wrecv[0].astype(F32)
        for s in range(1, slots):
            weight_sum = weight_sum + wrecv[s].astype(F32)
        w_ref[...] = weight_sum

    pl.run_scoped(body, pltpu.SemaphoreType.DMA((LOADS + len(RECEIVED),)))


def writer(qg, pg, w, qg_out, pg_out, w_out, sems):
    copies = [
        pltpu.make_async_copy(pg, pg_out, sems.at[0]),
        pltpu.make_async_copy(qg, qg_out, sems.at[1]),
        pltpu.make_async_copy(w, w_out, sems.at[2]),
    ]
    for c in copies:
        c.start()
    for c in copies:
        c.wait()


def shards(PB, PA, query_hidden, page_hidden, projection, clicks, bins):
    queries, token_local, hidden = query_hidden.shape
    page_count, patches, _ = page_hidden.shape
    assert page_count == 1 and PB % 2 == 0
    E = projection.shape[1]
    rows = queries * token_local
    half = PB // 2
    slots = half * PA
    tokens = rows * slots
    chunk = hidden // (PB * PA)
    span = PA * chunk
    pairs = clicks.shape[1]
    ph = page_hidden.reshape(patches, hidden)
    vmem = pl.BlockSpec(memory_space=pltpu.VMEM)
    hbm = pl.BlockSpec(memory_space=pltpu.HBM)
    dma = lambda n: pltpu.SemaphoreType.DMA((n,))
    outs = (
        jax.ShapeDtypeStruct(query_hidden.shape, BF),
        jax.ShapeDtypeStruct((patches, hidden), BF),
        jax.ShapeDtypeStruct((chunk, E), F32),
    )
    results = pl.pallas_call(
        functools.partial(kernel, PB, PA),
        out_shape=tuple(pltpu.VMEM(o.shape, o.dtype) for o in outs),
        in_specs=[hbm] * 5,
        out_specs=(vmem,) * 3,
        scratch_shapes=[
            pltpu.VMEM((half, queries, 2, pairs), jnp.int32),
            pltpu.VMEM((half, queries, pairs), jnp.int32),
            pltpu.VMEM(query_hidden.shape, BF),
            pltpu.VMEM((rows, hidden), F32),
            pltpu.VMEM((rows, hidden), BF),
            pltpu.VMEM((half, rows, span), BF),
            pltpu.VMEM((half, span, 2 * rows), BF),
            pltpu.VMEM((patches, hidden), BF),
            pltpu.VMEM((half, patches, span), BF),
            pltpu.VMEM((half, 2, span, patches), BF),
            pltpu.VMEM((hidden, E), BF),
            pltpu.VMEM((slots, rows, E), BF),
            pltpu.VMEM((E, tokens), F32),
            pltpu.VMEM((2, patches, E), BF),
            pltpu.VMEM((max(half - 1, 1), 2, patches, E), BF),
            pltpu.VMEM((2, patches, PA * rows), F32),
            pltpu.VMEM((2, patches, tokens), BF),
            pltpu.VMEM((2, tokens, patches), BF),
            pltpu.VMEM((max(half - 1, 1), 2, patches, PA * rows), BF),
            pltpu.VMEM((1, tokens), F32),
            pltpu.VMEM((1, tokens), F32),
            pltpu.VMEM((slots, 1, PA * rows), F32),
            pltpu.VMEM((PA, rows, E), BF),
            pltpu.VMEM((PA, rows, E), BF),
            pltpu.VMEM((2, E, patches), BF),
            pltpu.VMEM((2, E, patches), BF),
            pltpu.VMEM((2, rows, E), BF),
            pltpu.VMEM((half, span, E), F32),
            pltpu.VMEM((slots, chunk, E), BF),
            pltpu.VMEM((slots, chunk, E), BF),
            dma(len(RECEIVED)),
        ],
        compiler_params=pltpu.CompilerParams(
            collective_id=0, has_side_effects=True, vmem_limit_bytes=65536000
        ),
        name="fused",
    )(query_hidden, ph, projection, jnp.transpose(clicks, (0, 2, 1)), bins)
    query_grad, page_grad, weight_grad = pl.pallas_call(
        writer,
        out_shape=outs,
        in_specs=[vmem] * 3,
        out_specs=(hbm,) * 3,
        scratch_shapes=[dma(3)],
        compiler_params=pltpu.CompilerParams(vmem_limit_bytes=4 * 1024 * 1024),
        name="writer",
    )(*results)
    return query_grad, page_grad.reshape(page_hidden.shape), weight_grad


def solution(mesh):
    return jax.shard_map(
        functools.partial(shards, mesh.shape["pb"], mesh.shape["pa"]),
        mesh=mesh,
        in_specs=(
            P("pb", "pa", None),
            P("pa", "pb", None),
            P(),
            P("pb", None, None),
            P("pb", None),
        ),
        out_specs=(P("pb", "pa", None), P("pa", "pb", None), P(("pb", "pa"), None)),
        check_vma=False,
    )
```

```python
import functools
import math

import jax
import jax.numpy as jnp
from jax import lax
from jax.experimental import pallas as pl
from jax.experimental.pallas import tpu as pltpu
from jax.sharding import PartitionSpec as P

sharpness = 0.25
MESH = pl.DeviceIdType.MESH
BF = jnp.bfloat16
F32 = jnp.float32
FOLDED = sharpness * math.log2(math.e)
RECEIVED = (
    "near", "far", "click", "bin", "page", "other", "hidden", "raw", "level", "norm", "token", "patch", "low", "weight",
)
LOADS = 5


def dot(x, y, dims):
    return lax.dot_general(x, y, (dims, ((), ())), preferred_element_type=F32)


def kernel(
    PB, PA, qh_hbm, ph_hbm, proj_hbm, clicks_hbm, bins_hbm,
    qg_ref, pg_ref, w_ref,
    clicks_ref, bins_ref, qraw, qh, qb, qx, qt2, ph, hx, pht, proj, qe, qt, pe, po, lbuf, ebuf, ebt, eo, tops, sums, norm,
    tsend, trecv, gsend, grecv, low, wq, wsend, wrecv, arrived,
):
    b = lax.axis_index("pb")
    a = lax.axis_index("pa")
    queries, token_local, hidden = qh_hbm.shape
    rows = queries * token_local
    patches = ph_hbm.shape[0]
    E = proj.shape[1]
    half = PB // 2
    slots = half * PA
    level_tokens = PA * rows
    tokens = half * level_tokens
    parity = lax.rem(b, 2)
    level = b // 2
    me = level * PA + a
    partner = (b + 1 - 2 * parity, a)
    chunk = w_ref.shape[0]
    span = PA * chunk
    width = 2 if PA < 32 else 4
    deep = PA // width
    z = a // width
    x = lax.rem(a, width)
    upper = z >= deep // 2
    group = PA // 2
    side = a // group

    def others(offsets, ascending=False):
        for i in range(deep):
            far = i if ascending else jnp.where(upper, i, deep - 1 - i)
            for k in offsets:
                to_level = lax.rem(level + k, half)
                for j in list(range(1, width)) + [0]:
                    to_z = far
                    if k == 0 and j == 0:
                        if i == deep - 1:
                            continue
                        up = i + jnp.where(i >= z, 1, 0)
                        down = deep - 1 - i - jnp.where(deep - 1 - i <= z, 1, 0)
                        to_z = up if ascending else jnp.where(upper, up, down)
                    yield to_level, to_z * width + lax.rem(x + j, width)

    every = list(range(1, half)) + [0]

    def device(to_level, to_a):
        return 2 * to_level + parity, to_a

    def across(k):
        to_level = lax.rem(level + k, half)
        return device(to_level, a), (2 * to_level + 1 - parity, a)

    barrier = pltpu.get_barrier_semaphore()
    for to in others([0]):
        pl.semaphore_signal(barrier, inc=1, device_id=device(*to), device_id_type=MESH)
    for k in range(1, half):
        for to in across(k):
            pl.semaphore_signal(barrier, inc=1, device_id=to, device_id_type=MESH)
    pl.semaphore_signal(barrier, inc=1, device_id=partner, device_id_type=MESH)

    def body(sent):
        def remote(kind, src, dst, to, received=None):
            pltpu.make_async_remote_copy(
                src_ref=src, dst_ref=dst, send_sem=sent.at[LOADS + RECEIVED.index(kind)],
                recv_sem=arrived.at[RECEIVED.index(kind)] if received is None else received,
                device_id=to, device_id_type=MESH,
            ).start()

        def receive(kind, ref):
            pltpu.make_async_copy(ref, ref, arrived.at[RECEIVED.index(kind)]).wait()

        def flush(kind, ref):
            pltpu.make_async_copy(ref, ref, sent.at[LOADS + RECEIVED.index(kind)]).wait()

        loads = [
            pltpu.make_async_copy(qh_hbm, qraw, sent.at[0]),
            pltpu.make_async_copy(proj_hbm, proj, sent.at[1]),
            pltpu.make_async_copy(ph_hbm, ph, sent.at[2]),
            pltpu.make_async_copy(clicks_hbm, clicks_ref.at[level], sent.at[3]),
            pltpu.make_async_copy(bins_hbm, bins_ref.at[level], sent.at[4]),
        ]
        for c in loads:
            c.start()
        loads[0].wait()
        for q in range(queries):
            qh[q * token_local:(q + 1) * token_local] = qraw[q].astype(F32)
        qb[...] = qh[...].astype(BF)
        loads[1].wait()
        qe[me] = dot(qb[...], proj[...], ((1,), (0,))).astype(BF)
        loads[2].wait()
        pe[0] = dot(ph[...], proj[...], ((1,), (0,))).astype(BF)
        pl.semaphore_wait(barrier, PA + 2 * (half - 1))
        for k in range(1, half):
            for to in across(k):
                remote("other", pe.at[0], po.at[k - 1, parity], to)
        for to in others([0]):
            other_side = jnp.where(to[1] // group == side, 0, 1)
            remote("near", qe.at[me], qe.at[me], device(*to), arrived.at[other_side])
        remote("page", pe.at[0], pe.at[1], partner)
        for k in range(1, half):
            to = across(k)[0]
            remote("click", clicks_hbm, clicks_ref.at[level], to)
            remote("bin", bins_hbm, bins_ref.at[level], to)

        def columns(l, core):
            return pl.ds(pl.multiple_of((2 * l + core) * span, 128), span)

        for l in range(half):
            remote("hidden", ph.at[:, columns(l, 1 - parity)], hx.at[l], partner)
            remote("raw", qb.at[:, columns(l, 1 - parity)], qx.at[l], partner)

        query_of = lax.broadcasted_iota(jnp.int32, (queries, level_tokens), 0)
        token_of = lax.broadcasted_iota(jnp.int32, (queries, level_tokens), 1)
        mask = jnp.where(query_of == lax.rem(token_of, rows) // token_local, 1.0, 0.0)
        for l in range(half):
            pht[l, 0] = ph[:, columns(l, parity)].T
        receive("hidden", hx)
        for l in range(half):
            pht[l, 1] = hx[l].T
        receive("raw", qx)
        for l in range(half):
            qt2[l, :, :rows] = qb[:, columns(l, parity)].T
            qt2[l, :, rows:] = qx[l].T

        def spread(pages, tok, store):
            top = None
            count = tok.shape[0]
            for k in range(2):
                block = dot(pages(k), tok, ((1,), (1,)))
                lbuf[k, :, :count] = block
                high = jnp.max(block, axis=0, keepdims=True)
                top = high if top is None else jnp.maximum(top, high)
            total = None
            for k in range(2):
                e = jnp.exp2((lbuf[k, :, :count] - top) * FOLDED)
                store(k, e.astype(BF))
                part = jnp.sum(e, axis=0, keepdims=True)
                total = part if total is None else total + part
            return sharpness * top, total

        def lanes_of(start, count):
            return pl.ds(pl.multiple_of(start * rows, 128), count * rows)

        def own_chip(start, count):
            lanes = lanes_of(start, count)

            def store(k, e):
                ebuf[k, :, lanes] = e

            tok = qe[pl.ds(start, count)].reshape(count * rows, E)
            tops[:, lanes], sums[:, lanes] = spread(lambda k: pe[k], tok, store)

        receive("page", pe.at[0])
        for kind, part in (("near", side), ("far", 1 - side)):
            start = level * PA + group * part
            receive(kind, qe.at[pl.ds(0, group - 1 if kind == "near" else group)])
            for k in range(1, half):
                batch = qe.at[pl.ds(start, group)]
                remote("level", batch, batch, across(k)[0])
            own_chip(start, group)
        here = lanes_of(level * PA, PA)
        highs, totals = [tops[:, here]], [sums[:, here]]
        if half > 1:
            receive("other", po)
        for g in range(half - 1):
            def store(k, e):
                eo[g, k] = e

            tok = qe[pl.ds(level * PA, PA)].reshape(level_tokens, E)
            high, total = spread(lambda k: po[g, k], tok, store)
            highs.append(high)
            totals.append(total)
        high = functools.reduce(jnp.maximum, highs)
        total = functools.reduce(jnp.add, [t * jnp.exp(h - high) for h, t in zip(highs, totals)])
        log_norm = high + jnp.log(total)
        norm[me] = log_norm
        for to in others(every):
            remote("norm", norm.at[me], norm.at[me], device(*to))

        unit = None
        for g in range(half):
            for k in range(2):
                if g:
                    part = dot(po[g - 1, k], eo[g - 1, k], ((0,), (0,)))
                else:
                    part = dot(pe[k], ebuf[k, :, here], ((0,), (0,)))
                part = part * jnp.exp(highs[g] - log_norm)
                unit = part if unit is None else unit + part
        unit = unit.T.astype(BF)
        for s in range(PA):
            tsend[s] = unit[s * rows:(s + 1) * rows]
        for to_level, to_a in others([0]):
            remote("token", tsend.at[to_a], trecv.at[a], device(to_level, to_a))
        trecv[a] = tsend[a]
        for k in range(2):
            ebt[k, lanes_of(level * PA, PA)] = ebuf[k, :, here].T
        if half > 1:
            receive("level", qe.at[pl.ds(0, (half - 1) * PA)])
        for g in range(1, half):
            start = lax.rem(level + g, half) * PA
            own_chip(start, PA)
            for k in range(2):
                ebt[k, lanes_of(start, PA)] = ebuf[k, :, lanes_of(start, PA)].T
        qt[...] = qe[...].reshape(tokens, E).astype(F32).T

        loads[3].wait()
        loads[4].wait()
        if half > 1:
            receive("click", clicks_ref.at[pl.ds(0, half - 1)])
            receive("bin", bins_ref.at[pl.ds(0, half - 1)])
        pos = [clicks_ref[l, :, 0, :] for l in range(half)]
        neg = [clicks_ref[l, :, 1, :] for l in range(half)]
        weight = [jnp.sqrt(bins_ref[l].astype(F32) + 1.0) for l in range(half)]

        receive("norm", norm.at[pl.ds(0, slots - 1)])
        coeff = []
        for l in range(half):
            rows_in = norm[l * PA:(l + 1) * PA].reshape(PA, level_tokens)
            gap = jnp.zeros(pos[l].shape, F32)
            away = jnp.zeros(pos[l].shape, F32)
            for p in range(PA):
                score = jnp.sum(mask * rows_in[p:p + 1], axis=1, keepdims=True)
                gap = gap + jnp.where(pos[l] == p, score, 0.0)
                away = away + jnp.where(neg[l] == p, score, 0.0)
            coeff.append(-weight[l] * jax.nn.sigmoid(away - gap))

        def score_grad(l, page):
            hits = (pos[l] == page).astype(F32) - (neg[l] == page).astype(F32)
            return jnp.sum(coeff[l] * hits, axis=1, keepdims=True)

        scaled = []
        for l in range(half):
            at = slice(l * level_tokens, (l + 1) * level_tokens)
            factor = jnp.sum(mask * score_grad(l, a), axis=0, keepdims=True)
            factor = factor * jnp.exp(tops[:, at] - norm[l * PA + a])
            scaled.append((qt[:, at] * factor).astype(BF))
        scaled = jnp.concatenate(scaled, axis=1)
        mine = []
        for k in range(2):
            part = dot(scaled, ebt[k], ((1,), (0,)))
            gsend[k] = part.astype(BF)
            remote("patch", gsend.at[k], grecv.at[k], partner)
            mine.append(part)

        column = lax.broadcasted_iota(jnp.int32, (queries, 128), 1)
        table = jnp.zeros((queries, 128), F32)
        for p in range(PA):
            grad = jnp.zeros((queries, 1), F32)
            for l in range(half):
                grad = grad + jnp.where(level == l, score_grad(l, p), 0.0)
            table = jnp.where(column == p, grad, table)
        row_of = lax.broadcasted_iota(jnp.int32, (rows, 128), 0) // token_local
        shares = jnp.zeros((rows, 128), F32)
        for q in range(queries):
            shares = jnp.where(row_of == q, table[q:q + 1], shares)
        receive("token", trecv.at[pl.ds(0, PA - 1)])
        token_own = None
        for p in range(PA):
            part = trecv[p].astype(F32) * shares[:, p:p + 1]
            token_own = part if token_own is None else token_own + part
        token_low = (sharpness * token_own).astype(BF)
        low[0] = token_low
        remote("low", low.at[0], low.at[1], partner)

        receive("low", low.at[0])
        for l in range(half):
            wq[l] = dot(qt2[l], low[...].reshape(2 * rows, E), ((1,), (0,)))

        receive("patch", grecv)
        patch_low = [(sharpness * (mine[k] + grecv[1 - k].astype(F32))).astype(BF).T for k in range(2)]

        for k in every:
            to_level = lax.rem(level + k, half)
            block = wq[to_level]
            for i in range(2):
                block = block + dot(pht[to_level, i], patch_low[i], ((1,), (0,)))
            block = block.astype(BF)
            for s in range(PA):
                wsend[to_level * PA + s] = block[s * chunk:(s + 1) * chunk]
        place = a * half + level
        for n in range(slots - 1):
            d = n + jnp.where(n >= place, 1, 0)
            to_level, to_a = lax.rem(d, half), d // half
            remote("weight", wsend.at[to_level * PA + to_a], wrecv.at[me], device(to_level, to_a))
        wrecv[me] = wsend[me]

        qgrad = dot(token_low, proj[...], ((1,), (1,)))
        for q in range(queries):
            qg_ref[q] = qgrad[q * token_local:(q + 1) * token_local].astype(BF)
        pg_ref[...] = dot(patch_low[0], proj[...], ((1,), (1,))).astype(BF)

        flush("near", qe.at[pl.ds(0, PA - 1)])
        if half > 1:
            flush("click", clicks_ref.at[pl.ds(0, half - 1)])
            flush("bin", bins_ref.at[pl.ds(0, half - 1)])
            flush("other", po)
            flush("level", qe.at[pl.ds(0, (half - 1) * PA)])
        flush("page", pe.at[0])
        flush("hidden", hx)
        flush("raw", qx)
        flush("norm", norm.at[pl.ds(0, slots - 1)])
        flush("token", tsend.at[pl.ds(0, PA - 1)])
        flush("patch", gsend)
        flush("low", low.at[0])
        flush("weight", wsend.at[pl.ds(0, slots - 1)])
        receive("weight", wrecv.at[pl.ds(0, slots - 1)])
        weight_sum = wrecv[0].astype(F32)
        for s in range(1, slots):
            weight_sum = weight_sum + wrecv[s].astype(F32)
        w_ref[...] = weight_sum

    pl.run_scoped(body, pltpu.SemaphoreType.DMA((LOADS + len(RECEIVED),)))


def writer(qg, pg, w, qg_out, pg_out, w_out, sems):
    copies = [
        pltpu.make_async_copy(pg, pg_out, sems.at[0]),
        pltpu.make_async_copy(qg, qg_out, sems.at[1]),
        pltpu.make_async_copy(w, w_out, sems.at[2]),
    ]
    for c in copies:
        c.start()
    for c in copies:
        c.wait()


def shards(PB, PA, query_hidden, page_hidden, projection, clicks, bins):
    queries, token_local, hidden = query_hidden.shape
    page_count, patches, _ = page_hidden.shape
    assert page_count == 1 and PB % 2 == 0
    E = projection.shape[1]
    rows = queries * token_local
    half = PB // 2
    slots = half * PA
    tokens = rows * slots
    chunk = hidden // (PB * PA)
    span = PA * chunk
    pairs = clicks.shape[1]
    ph = page_hidden.reshape(patches, hidden)
    vmem = pl.BlockSpec(memory_space=pltpu.VMEM)
    hbm = pl.BlockSpec(memory_space=pltpu.HBM)
    dma = lambda n: pltpu.SemaphoreType.DMA((n,))
    outs = (
        jax.ShapeDtypeStruct(query_hidden.shape, BF),
        jax.ShapeDtypeStruct((patches, hidden), BF),
        jax.ShapeDtypeStruct((chunk, E), F32),
    )
    results = pl.pallas_call(
        functools.partial(kernel, PB, PA),
        out_shape=tuple(pltpu.VMEM(o.shape, o.dtype) for o in outs),
        in_specs=[hbm] * 5,
        out_specs=(vmem,) * 3,
        scratch_shapes=[
            pltpu.VMEM((half, queries, 2, pairs), jnp.int32),
            pltpu.VMEM((half, queries, pairs), jnp.int32),
            pltpu.VMEM(query_hidden.shape, BF),
            pltpu.VMEM((rows, hidden), F32),
            pltpu.VMEM((rows, hidden), BF),
            pltpu.VMEM((half, rows, span), BF),
            pltpu.VMEM((half, span, 2 * rows), BF),
            pltpu.VMEM((patches, hidden), BF),
            pltpu.VMEM((half, patches, span), BF),
            pltpu.VMEM((half, 2, span, patches), BF),
            pltpu.VMEM((hidden, E), BF),
            pltpu.VMEM((slots, rows, E), BF),
            pltpu.VMEM((E, tokens), F32),
            pltpu.VMEM((2, patches, E), BF),
            pltpu.VMEM((max(half - 1, 1), 2, patches, E), BF),
            pltpu.VMEM((2, patches, PA * rows), F32),
            pltpu.VMEM((2, patches, tokens), BF),
            pltpu.VMEM((2, tokens, patches), BF),
            pltpu.VMEM((max(half - 1, 1), 2, patches, PA * rows), BF),
            pltpu.VMEM((1, tokens), F32),
            pltpu.VMEM((1, tokens), F32),
            pltpu.VMEM((slots, 1, PA * rows), F32),
            pltpu.VMEM((PA, rows, E), BF),
            pltpu.VMEM((PA, rows, E), BF),
            pltpu.VMEM((2, E, patches), BF),
            pltpu.VMEM((2, E, patches), BF),
            pltpu.VMEM((2, rows, E), BF),
            pltpu.VMEM((half, span, E), F32),
            pltpu.VMEM((slots, chunk, E), BF),
            pltpu.VMEM((slots, chunk, E), BF),
            dma(len(RECEIVED)),
        ],
        compiler_params=pltpu.CompilerParams(
            collective_id=0, has_side_effects=True, vmem_limit_bytes=65536000
        ),
        name="fused",
    )(query_hidden, ph, projection, jnp.transpose(clicks, (0, 2, 1)), bins)
    query_grad, page_grad, weight_grad = pl.pallas_call(
        writer,
        out_shape=outs,
        in_specs=[vmem] * 3,
        out_specs=(hbm,) * 3,
        scratch_shapes=[dma(3)],
        compiler_params=pltpu.CompilerParams(vmem_limit_bytes=4 * 1024 * 1024),
        name="writer",
    )(*results)
    return query_grad, page_grad.reshape(page_hidden.shape), weight_grad


def solution(mesh):
    return jax.shard_map(
        functools.partial(shards, mesh.shape["pb"], mesh.shape["pa"]),
        mesh=mesh,
        in_specs=(
            P("pb", "pa", None),
            P("pa", "pb", None),
            P(),
            P("pb", None, None),
            P("pb", None),
        ),
        out_specs=(P("pb", "pa", None), P("pa", "pb", None), P(("pb", "pa"), None)),
        check_vma=False,
    )
```
